32 devices in a mesh: dp: 8 (over z, y), neg: 4 (over x, core).
Axes of the slice: x: 2, y: 2, z: 4, core: 2. Of those that a mesh axis runs over, the one named last changes fastest.
Arguments:
- user_embed: bfloat16 [24576, 256], P(('dp', 'neg')), may hold values from -25 to 25
- positive_embed: bfloat16 [24576, 256], P(('dp', 'neg')), may hold values from -6 to 6
- positive_ids: int32 [24576], P(('dp', 'neg')), may hold values from 0 to 1048575
- token_weights: int32 [24576], P(('dp', 'neg')), may hold values from 1 to 5
- offsets: int32 [8, 25], P('dp'), may hold values from 0 to 3072, as said below
- negative_embed: bfloat16 [32768, 256], P('neg'), may hold values from -6 to 6
- negative_ids: int32 [32768], P('neg'), may hold values from 0 to 1048575
Outputs:
- token_loss: float32 [24576], P(('dp', 'neg'))
- mean_loss: float32 [], replicated
The draws below stay inside these ranges and needn't reach their ends.
Inputs may be any that keep to these rules, and one draw needn't show every extreme that they name: `offsets`: each row starts at 0 and does not fall; every user holds 2 or more slots; in every draw some group fills all 3072 slots.
All inputs are finite; a program needn't handle non-finite values.
Results may differ from the reference program's by a relative error of at most 0.0003.
Values may be sent and summed in bfloat16 or wider, within the bound.
No kernel may reach another device: no remote copies, remote signals or barrier semaphores. Data moves between devices by JAX's collectives and lax.ppermute only.
A program may use at most 64 MiB of HBM per device.

```python
import math
import jax
import jax.numpy as jnp
from jax import lax

D = 256
NEG_DEV = 8192
TOK_DEV = 768
USERS = 24
ITEMS = 1048576
NEGS = 32768
TOKENS = 24576
N_DP = 8
N_NEG = 4


def drawn_slots(key):
    base = jax.random.fold_in(key, 13)
    chosen = jax.random.permutation(jax.random.fold_in(base, 1), NEGS // 2)[:32].astype(jnp.int32)
    picked = (2 * NEG_DEV * (chosen // NEG_DEV) + chosen % NEG_DEV).astype(jnp.int32)
    partner = (picked + NEG_DEV).astype(jnp.int32)
    strengths = jax.random.uniform(jax.random.fold_in(base, 2), (32,), jnp.float32, 6.0, 10.0)
    targets = jax.random.permutation(jax.random.fold_in(base, 3), TOKENS)[:32].astype(jnp.int32)
    return (picked, partner, strengths, targets)


def negative_table(key):
    base = jax.random.fold_in(key, 11)
    table = jnp.clip(jax.random.normal(base, (NEGS, D), jnp.float32), -6.0, 6.0)
    return table


def draw_negative_embed(key, part):
    return negative_table(key).astype(jnp.bfloat16)


def draw_user_embed(key, part):
    base = jax.random.fold_in(key, 17)
    table = negative_table(key)
    picked, partner, strengths, targets = drawn_slots(key)
    rows = jnp.clip(jax.random.normal(base, (TOKENS, D), jnp.float32), -6.0, 6.0)
    rows = rows.at[targets].set(0.25 * strengths[:, None] * table[picked])
    return rows.astype(jnp.bfloat16)


def item_ids(key, salt, number):
    mixing = jax.random.fold_in(key, 5)
    factor = jax.random.randint(jax.random.fold_in(mixing, 1), (), 0, 1024) * 2 + 1
    offset = jax.random.randint(jax.random.fold_in(mixing, 2), (), 0, ITEMS)
    base = jax.random.fold_in(key, salt)
    levels = jax.random.randint(jax.random.fold_in(base, 1), (number,), 0, 21)
    upper = jnp.left_shift(jnp.ones((number,), jnp.int32), levels)
    raw = jax.random.randint(jax.random.fold_in(base, 2), (number,), 0, upper)
    return jnp.bitwise_and(raw * factor + offset, ITEMS - 1).astype(jnp.int32)


def draw_positive_ids(key, part):
    return item_ids(key, 21, TOKENS)


def draw_negative_ids(key, part):
    values = item_ids(key, 23, NEGS)
    picked, partner, strengths, targets = drawn_slots(key)
    wanted = item_ids(key, 21, TOKENS)[targets[:16]]
    values = values.at[picked[:16]].set(wanted)
    values = values.at[partner[:16]].set(wanted)
    return values.astype(jnp.int32)


def draw_offsets(key, part):
    base = jax.random.fold_in(key, 29)
    group_size = TOK_DEV * N_NEG
    groups = jnp.arange(N_DP, dtype=jnp.int32)
    start_live = group_size * (N_DP + 2 * groups) // (3 * N_DP)
    jitter = jax.random.randint(jax.random.fold_in(base, 1), (N_DP,), 0, group_size // 16 + 1)
    live = jnp.maximum(start_live - jitter, 2 * USERS)
    filled = jax.random.randint(jax.random.fold_in(base, 2), (), 0, N_DP)
    live = jnp.where(groups == filled, group_size, live)
    cuts = jax.random.randint(jax.random.fold_in(base, 3), (N_DP, USERS - 1), 0, (live - 2 * USERS + 1)[:, None])
    cuts = jnp.sort(cuts, axis=1)
    middle = cuts + 2 * jnp.arange(1, USERS, dtype=jnp.int32)[None, :]
    zeros_col = jnp.zeros((N_DP, 1), jnp.int32)
    return jnp.concatenate([zeros_col, middle, live[:, None]], axis=1).astype(jnp.int32)


def with_ends(drawn, key, smallest, top_value):
    longest = drawn.shape.index(max(drawn.shape))
    spots = []
    for shift in (0, 1):
        where = [jax.random.randint(jax.random.fold_in(key, axis), (), 0, length) for axis, length in enumerate(drawn.shape)]
        where[longest] = (where[longest] + shift) % drawn.shape[longest]
        spots.append(tuple(where))
    return drawn.at[spots[0]].set(smallest).at[spots[1]].set(top_value)


def block_scale(key, extent, cuts, smallest, largest):
    level = 1.0
    for position, shards_of in cuts:
        draws = jax.random.uniform(jax.random.fold_in(jax.random.fold_in(key, 6), position), (shards_of,), jnp.float32, smallest / len(cuts), largest / len(cuts))
        level = level * jnp.repeat(jnp.exp(draws), extent[position] // shards_of).reshape((-1,) + (1,) * (len(extent) - 1 - position))
    return level


def scatter_about(rng, shape, spread, most, pieces=(), kind=jnp.bfloat16):
    values = jax.random.normal(rng, shape, jnp.float32) * spread
    if len(pieces) > 0:
        values = block_scale(rng, shape, pieces, -0.22, 0.18) * values
    return jnp.clip(values, min=-most, max=most).astype(kind)


def setup_inputs(seed: int = 0) -> dict:
    arg_keys = jax.random.split(jax.random.key(seed), 8)
    return {
        "user_embed": draw_user_embed(jax.random.fold_in(arg_keys[7], 71), 0),
        "positive_embed": scatter_about(arg_keys[1], (TOKENS, D), 1.0, 6.0, ((0, 32),)),
        "positive_ids": draw_positive_ids(jax.random.fold_in(arg_keys[7], 71), 0),
        "token_weights": with_ends(jax.random.randint(arg_keys[3], (TOKENS,), 1, 6), jax.random.fold_in(arg_keys[3], 1), 1, 5).astype(jnp.int32),
        "offsets": draw_offsets(jax.random.fold_in(arg_keys[7], 71), 0),
        "negative_embed": draw_negative_embed(jax.random.fold_in(arg_keys[7], 71), 0),
        "negative_ids": draw_negative_ids(jax.random.fold_in(arg_keys[7], 71), 0),
    }


def reference(user_embed, positive_embed, positive_ids, token_weights, offsets, negative_embed, negative_ids):
    scale = 3.0 / math.sqrt(D)
    block = math.gcd(TOKENS, 512)
    users_blocks = user_embed.reshape(TOKENS // block, block, D)
    pos_blocks = positive_embed.reshape(TOKENS // block, block, D)
    ids_blocks = positive_ids.reshape(TOKENS // block, block)

    def one_block(triple):
        rows, pos_rows, row_ids = triple
        logits = jnp.dot(rows, negative_embed.T, preferred_element_type=jnp.float32) * scale
        positive = lax.optimization_barrier(jnp.sum(rows.astype(jnp.float32) * pos_rows.astype(jnp.float32), axis=1)) * scale
        hit = row_ids[:, None] == negative_ids[None, :]
        masked = jnp.where(hit, -jnp.inf, logits)
        peak = jnp.maximum(lax.optimization_barrier(jnp.max(masked, axis=1)), positive)
        summed = lax.optimization_barrier(jnp.sum(jnp.exp(masked - peak[:, None]), axis=1)) + jnp.exp(positive - peak)
        return peak + jnp.log(summed) - positive
    losses = lax.map(one_block, (users_blocks, pos_blocks, ids_blocks)).reshape(TOKENS)
    group_size = TOKENS // N_DP
    positions = jnp.arange(group_size, dtype=jnp.int32)
    ends = offsets[:, 1:]
    last_slot = jnp.any(positions[None, :, None] + 1 == ends[:, None, :], axis=2)
    live = (positions[None, :] < offsets[:, USERS:USERS + 1]) & jnp.logical_not(last_slot)
    live = live.reshape(TOKENS)
    token_loss = jnp.where(live, losses, jnp.float32(0.0)).astype(jnp.float32)
    weight = token_weights.astype(jnp.float32)
    total = jnp.sum(weight * token_loss)
    count = jnp.sum(weight * live.astype(jnp.float32))
    return (token_loss, total / count)
```

```python
import functools
import math

import jax
import jax.numpy as jnp
from jax import lax
from jax.experimental import pallas as pl
from jax.experimental.pallas import tpu as pltpu
from jax.sharding import PartitionSpec as P

LANES = 128
TILE = 256
BLOCK = 512
ID_ROWS = 16
LOG2E = math.log2(math.e)
FLOOR = -1e30
HIGHEST = 2.0**126
LOWEST = 2.0**-90
CONTRACT = (((1,), (1,)), ((), ()))


def tile_ids(packs, pack, tile, tiles, tokens):
    digits = packs[pack][tokens : tokens + ID_ROWS, :].astype(jnp.float32)
    rows = [digits[d * tiles + tile : d * tiles + tile + 1] for d in range(3)]
    return rows[0] + 128.0 * rows[1] + 16384.0 * rows[2]


def partial_kernel(scale2, tokens, count, *refs):
    packs = refs[:count]
    negs, id_table, id_rows, out, sums, ids, bad_ref, logits = refs[count:]
    number = negs.shape[0]
    tiles = tokens // TILE
    for pack in range(count):
        for tile in range(tiles):
            ids[pack * tiles + tile] = jnp.broadcast_to(
                tile_ids(packs, pack, tile, tiles, tokens), (8, TILE)
            ).astype(jnp.int32)

    for pack in range(count):

        def one_tile(tile, _, pack=pack):
            slot = pack * tiles + tile
            rhs = packs[pack][pl.ds(pl.multiple_of(tile * TILE, TILE), TILE), :]
            wanted = ids[slot]
            halves = [jnp.zeros((8, LANES), jnp.float32) for _ in range(2)]
            for start in range(0, number, BLOCK):
                size = min(BLOCK, number - start)
                rows = pl.ds(start, size)
                logit = lax.dot_general(
                    negs[rows, :], rhs, CONTRACT, preferred_element_type=jnp.float32
                )
                grown = jnp.exp2(logit * scale2)
                ids_here = id_table[rows, :].reshape(size // 8, 8, LANES)
                for half in range(2):
                    lanes = slice(half * LANES, (half + 1) * LANES)
                    part = grown[:, lanes].reshape(size // 8, 8, LANES)
                    part = jnp.where(ids_here == wanted[None, :, lanes], 0.0, part)
                    halves[half] = halves[half] + part.sum(0)
            for half in range(2):
                sums[slot, :, half * LANES : (half + 1) * LANES] = halves[half]
            return 0

        lax.fori_loop(0, tiles, one_tile, 0)

    slots = count * tiles
    worst = jnp.zeros((1, TILE), jnp.float32)
    for slot in range(slots):
        total = jnp.sum(sums[slot], axis=0, keepdims=True)
        good = (total < HIGHEST) & (total > LOWEST)
        bad = jnp.where(good, 0.0, 1.0)
        worst = jnp.maximum(worst, bad)
        bad_ref[slot] = jnp.broadcast_to(bad, (16, TILE))
        value = jnp.log2(jnp.where(good, total, 1.0))
        out[2 * slot : 2 * slot + 1, :] = value[:, :LANES]
        out[2 * slot + 1 : 2 * slot + 2, :] = value[:, LANES:]

    @pl.when(jnp.max(worst) > 0.0)
    def _():
        lower = lax.broadcasted_iota(jnp.int32, (TILE, TILE), 0)
        upper = lax.broadcasted_iota(jnp.int32, (TILE, TILE), 1)
        triangle = jnp.where(lower <= upper, 1.0, 0.0).astype(jnp.bfloat16)
        for pack in range(count):

            def redo_tile(tile, _, pack=pack):
                slot = pack * tiles + tile
                bad = bad_ref[slot]
                rank = lax.dot_general(
                    bad.astype(jnp.bfloat16),
                    triangle,
                    (((1,), (0,)), ((), ())),
                    preferred_element_type=jnp.float32,
                )
                here = jnp.max(rank).astype(jnp.int32)
                block = packs[pack][pl.ds(pl.multiple_of(tile * TILE, TILE), TILE), :]
                wanted = ids[slot][0:1].astype(jnp.float32)

                def batch(b, _):
                    places = lax.broadcasted_iota(jnp.int32, (16, TILE), 0) + (1 + 16 * b)
                    chosen = (rank == places.astype(jnp.float32)) & (bad > 0.0)
                    pick = jnp.where(chosen, 1.0, 0.0)
                    rows = lax.dot_general(
                        pick.astype(jnp.bfloat16),
                        block,
                        (((1,), (0,)), ((), ())),
                        preferred_element_type=jnp.float32,
                    ).astype(jnp.bfloat16)
                    mine = jnp.sum(pick * wanted, axis=1, keepdims=True)

                    def score(c, peak):
                        part = lax.dot_general(
                            rows,
                            negs[pl.ds(pl.multiple_of(c * 1024, 1024), 1024), :],
                            CONTRACT,
                            preferred_element_type=jnp.float32,
                        )
                        part = part * scale2
                        others = id_rows[pl.ds(pl.multiple_of(c * 8, 8), 8), :].astype(jnp.float32)
                        for k in range(8):
                            piece = part[:, k * LANES : (k + 1) * LANES]
                            piece = jnp.where(others[k : k + 1] == mine, FLOOR, piece)
                            logits[c * 8 + k] = piece
                            peak = jnp.maximum(peak, piece)
                        return peak

                    peak = lax.fori_loop(
                        0, number // 1024, score, jnp.full((16, LANES), FLOOR, jnp.float32)
                    )
                    peak = jnp.max(peak, axis=1, keepdims=True)

                    def add(c, total):
                        piece = logits[c]
                        return total + jnp.where(
                            piece > 0.5 * FLOOR, jnp.exp2(piece - peak), 0.0
                        )

                    total = lax.fori_loop(
                        0, number // LANES, add, jnp.zeros((16, LANES), jnp.float32)
                    )
                    total = jnp.sum(total, axis=1, keepdims=True)
                    value = jnp.where(
                        total > 0.0, peak + jnp.log2(jnp.where(total > 0.0, total, 1.0)), FLOOR
                    )
                    spread = jnp.sum(pick * value, axis=0, keepdims=True)
                    took = jnp.sum(pick, axis=0, keepdims=True) > 0.0
                    for half in range(2):
                        lanes = slice(half * LANES, (half + 1) * LANES)
                        row = pl.ds(2 * slot + half, 1)
                        out[row, :] = jnp.where(took[:, lanes], spread[:, lanes], out[row, :])
                    return 0

                lax.fori_loop(0, (here + 15) // 16, batch, 0)
                return 0

            lax.fori_loop(0, tiles, redo_tile, 0)


def partials(scale2, tokens, packs, negs, id_table, id_rows):
    count = len(packs)
    number = negs.shape[0]
    slots = count * (tokens // TILE)
    vmem = pl.BlockSpec(memory_space=pltpu.VMEM)
    return pl.pallas_call(
        functools.partial(partial_kernel, scale2, tokens, count),
        out_shape=jax.ShapeDtypeStruct((2 * slots, LANES), jnp.float32),
        in_specs=[vmem] * (count + 3),
        out_specs=vmem,
        scratch_shapes=[
            pltpu.VMEM((slots, 8, TILE), jnp.float32),
            pltpu.VMEM((slots, 8, TILE), jnp.int32),
            pltpu.VMEM((slots, 16, TILE), jnp.float32),
            pltpu.VMEM((number // LANES, 16, LANES), jnp.float32),
        ],
        compiler_params=pltpu.CompilerParams(vmem_limit_bytes=24 * 2**20),
        cost_estimate=pl.CostEstimate(
            flops=2 * count * tokens * number * negs.shape[1],
            bytes_accessed=number * negs.shape[1] * 2,
            transcendentals=count * tokens * number,
        ),
    )(*packs, negs, id_table, id_rows)


def finish_kernel(members, rows, me, gathered, loss_out, totals_out):
    weighted = jnp.zeros((rows, LANES), jnp.float32)
    counted = jnp.zeros((rows, LANES), jnp.float32)
    own = jnp.zeros((rows, LANES), jnp.float32)
    for owner in range(members):
        positive = gathered[owner, members * rows : (members + 1) * rows, :]
        weight = gathered[owner, (members + 1) * rows : (members + 2) * rows, :]
        shares = [
            gathered[k, (owner ^ k) * rows : ((owner ^ k) + 1) * rows, :] for k in range(members)
        ]
        peak = positive
        for share in shares:
            peak = jnp.maximum(peak, share)
        total = jnp.exp2(positive - peak)
        for share in shares:
            total = total + jnp.exp2(share - peak)
        loss = (peak - positive + jnp.log2(total)) * (1.0 / LOG2E)
        loss = jnp.where(weight > 0.0, loss, 0.0)
        weighted = weighted + weight * loss
        counted = counted + weight
        own = jnp.where(me[0] == owner, loss, own)
    loss_out[...] = own
    first = jnp.sum(weighted, axis=0, keepdims=True)
    second = jnp.sum(counted, axis=0, keepdims=True)
    line = lax.broadcasted_iota(jnp.int32, (8, LANES), 0)
    totals_out[...] = jnp.where(line == 0, first, jnp.where(line == 1, second, 0.0))


def exchanged(value, axis, size, mask):
    return lax.ppermute(value, axis, [(i, i ^ mask) for i in range(size)])


def shards(
    dp,
    members,
    user_embed,
    positive_embed,
    positive_ids,
    token_weights,
    offsets,
    negative_embed,
    negative_ids,
):
    tokens, width = user_embed.shape
    number = negative_embed.shape[0]
    tiles = tokens // TILE
    rows = tokens // LANES
    scale = 3.0 / math.sqrt(width)
    me = lax.axis_index("neg")

    places = positive_ids.reshape(tiles, TILE)
    digits = jnp.concatenate([places & 127, (places >> 7) & 127, places >> 14], axis=0)
    digits = jnp.pad(digits, ((0, ID_ROWS - 3 * tiles), (0, 0))).astype(jnp.bfloat16)
    pack = jnp.concatenate([user_embed, digits], axis=0)
    id_table = jnp.broadcast_to(negative_ids[:, None], (number, LANES))
    id_rows = negative_ids.reshape(number // LANES, LANES)

    run = functools.partial(partials, scale * LOG2E, tokens)
    packs = [pack, exchanged(pack, "neg", members, 1)]
    for mask in [2**k for k in range(1, members.bit_length() - 1)]:
        packs += [exchanged(pack, "neg", members, mask)] + [None] * (mask - 1)
    shares = [run(packs[:2], negative_embed, id_table, id_rows)]
    for mask in range(2, members):
        if packs[mask] is None:
            low = mask & -mask
            source, shares[0] = lax.optimization_barrier((packs[mask ^ low], shares[0]))
            packs[mask] = exchanged(source, "neg", members, low)
    for mask in range(2, members):
        shares.append(run(packs[mask : mask + 1], negative_embed, id_table, id_rows))

    positions = me * tokens + jnp.arange(tokens, dtype=jnp.int32)
    ends = offsets[0, 1:]
    last_slot = jnp.any(positions[:, None] + 1 == ends[None, :], axis=1)
    live = (positions < offsets[0, -1]) & jnp.logical_not(last_slot)
    weight = jnp.where(live, token_weights, 0).astype(jnp.float32)
    positive = jnp.sum(
        user_embed.astype(jnp.float32) * positive_embed.astype(jnp.float32), axis=1
    ) * (scale * LOG2E)
    payload = jnp.concatenate(
        shares + [positive.reshape(rows, LANES), weight.reshape(rows, LANES)], axis=0
    )
    gathered = lax.all_gather(payload, "neg", axis=0)
    vmem = pl.BlockSpec(memory_space=pltpu.VMEM)
    loss, totals = pl.pallas_call(
        functools.partial(finish_kernel, members, rows),
        out_shape=(
            jax.ShapeDtypeStruct((rows, LANES), jnp.float32),
            jax.ShapeDtypeStruct((8, LANES), jnp.float32),
        ),
        in_specs=[pl.BlockSpec(memory_space=pltpu.SMEM), vmem],
        out_specs=(vmem, vmem),
    )(me.reshape(1).astype(jnp.int32), gathered)
    mask = 1
    while mask < dp:
        totals = totals + exchanged(totals, "dp", dp, mask)
        mask *= 2
    mean = jnp.sum(totals[0]) / jnp.sum(totals[1])
    return (loss.reshape(tokens), mean)


def solution(mesh):
    dp, members = mesh.shape["dp"], mesh.shape["neg"]
    in_specs = (
        P(("dp", "neg"), None),
        P(("dp", "neg"), None),
        P(("dp", "neg")),
        P(("dp", "neg")),
        P("dp", None),
        P("neg", None),
        P("neg"),
    )
    out_specs = (P(("dp", "neg")), P())
    return jax.shard_map(
        functools.partial(shards, dp, members),
        mesh=mesh,
        in_specs=in_specs,
        out_specs=out_specs,
        check_vma=False,
    )
```

```python
import functools
import math

import jax
import jax.numpy as jnp
from jax import lax
from jax.experimental import pallas as pl
from jax.experimental.pallas import tpu as pltpu
from jax.sharding import PartitionSpec as P

LANES = 128
TILE = 256
BLOCK = 512
ID_ROWS = 16
BATCH = 16
LOG2E = math.log2(math.e)
FLOOR = -1e30
HIGHEST = 2.0**126
LOWEST = 2.0**-90
CONTRACT = (((1,), (1,)), ((), ()))
VMEM = pl.BlockSpec(memory_space=pltpu.VMEM)
SMEM = pl.BlockSpec(memory_space=pltpu.SMEM)


def pack_kernel(users, places, out):
    tokens = users.shape[0]
    tiles = tokens // TILE
    out[0:tokens, :] = users[...]
    ids = places[...]
    lines = []
    for digit in (ids & 127, (ids >> 7) & 127, ids >> 14):
        digit = digit.astype(jnp.float32)
        for tile in range(tiles):
            lines.append(
                jnp.concatenate(
                    [digit[2 * tile : 2 * tile + 1], digit[2 * tile + 1 : 2 * tile + 2]], axis=1
                )
            )
    lines.append(jnp.zeros((ID_ROWS - len(lines), TILE), jnp.float32))
    out[tokens:, :] = jnp.concatenate(lines, axis=0).astype(out.dtype)


def tile_ids(pack, tile):
    tokens = pack.shape[0] - ID_ROWS
    tiles = tokens // TILE
    digits = pack[tokens:, :].astype(jnp.float32)
    rows = [digits[d * tiles + tile : d * tiles + tile + 1] for d in range(3)]
    return rows[0] + 128.0 * rows[1] + 16384.0 * rows[2]


def sum_pack(scale2, pack, negs, id_rows, out, first):
    tokens = pack.shape[0] - ID_ROWS
    number = negs.shape[0]
    tiles = tokens // TILE
    wanted = [
        jnp.broadcast_to(tile_ids(pack, tile), (8, TILE)).astype(jnp.int32) for tile in range(tiles)
    ]
    totals = [jnp.zeros((8, LANES), jnp.float32) for _ in range(2 * tiles)]
    for start in range(0, number, BLOCK):
        size = min(BLOCK, number - start)
        block = negs[pl.ds(start, size), :]
        others = [
            jnp.broadcast_to(id_rows[row : row + 1, :], (LANES, LANES)).T
            for row in range(start // LANES, (start + size) // LANES)
        ]
        others = jnp.concatenate(others, axis=0).reshape(size // 8, 8, LANES)
        for tile in range(tiles):
            users = pack[tile * TILE : (tile + 1) * TILE, :]
            logit = lax.dot_general(block, users, CONTRACT, preferred_element_type=jnp.float32)
            grown = jnp.exp2(logit * scale2)
            for half in range(2):
                lanes = slice(half * LANES, (half + 1) * LANES)
                part = grown[:, lanes].reshape(size // 8, 8, LANES)
                part = jnp.where(others == wanted[tile][None, :, lanes], 0.0, part)
                totals[2 * tile + half] = totals[2 * tile + half] + part.sum(0)
    for row in range(2 * tiles):
        out[first + row : first + row + 1, :] = jnp.sum(totals[row], axis=0, keepdims=True)


def sums_kernel(scale2, count, *refs):
    packs, (negs, id_rows, out) = refs[:count], refs[count:]
    rows = (packs[0].shape[0] - ID_ROWS) // LANES
    for k, pack in enumerate(packs):
        sum_pack(scale2, pack, negs, id_rows, out, k * rows)


def side_kernel(scale2, me, offsets, pack, targets, weights, out):
    tokens = targets.shape[0]
    rows = tokens // LANES
    product = pack[0:tokens, :].astype(jnp.float32) * targets[...].astype(jnp.float32)
    high = product.astype(jnp.bfloat16)
    low = (product - high.astype(jnp.float32)).astype(jnp.bfloat16)
    ones = jnp.ones((16, product.shape[1]), jnp.bfloat16)
    positive = lax.dot_general(
        ones, high, CONTRACT, preferred_element_type=jnp.float32
    ) + lax.dot_general(ones, low, CONTRACT, preferred_element_type=jnp.float32)
    positive = positive * scale2
    for row in range(rows):
        out[row : row + 1, :] = positive[0:1, row * LANES : (row + 1) * LANES]
    line = lax.broadcasted_iota(jnp.int32, (rows, LANES), 0)
    lane = lax.broadcasted_iota(jnp.int32, (rows, LANES), 1)
    position = me[0] * tokens + line * LANES + lane
    users = offsets.shape[1]
    live = position < offsets[0, users - 1]
    for user in range(1, users):
        live = live & (position + 1 != offsets[0, user])
    out[rows:, :] = jnp.where(live, weights[...], 0).astype(jnp.float32)


def last_kernel(scale2, members, *refs):
    packs = refs[:members]
    negs, id_rows, *rest = refs[members:]
    early, side, out, sums, chosen, picked, mine, logits, values = (
        rest[: members - 2],
        *rest[members - 2 :],
    )
    tokens = packs[0].shape[0] - ID_ROWS
    number = negs.shape[0]
    rows = tokens // LANES
    lines = members * rows
    first = 0
    for share in early:
        sums[first : first + share.shape[0], :] = share[...]
        first += share.shape[0]
    sum_pack(scale2, packs[-1], negs, id_rows, sums, first)
    total = sums[...]
    good = (total < HIGHEST) & (total > LOWEST)
    out[0:lines, :] = jnp.log2(jnp.where(good, total, 1.0))
    out[lines:, :] = side[...]
    bad = jnp.where(good, 0.0, 1.0)

    @pl.when(jnp.max(bad) > 0.0)
    def _():
        place = lax.broadcasted_iota(jnp.int32, (lines, LANES), 0) * LANES
        place = (place + lax.broadcasted_iota(jnp.int32, (lines, LANES), 1)).astype(jnp.float32)
        beyond = float(lines * LANES)
        sums[...] = jnp.where(good, beyond, place)
        wanted = []
        for pack in packs:
            for tile in range(tokens // TILE):
                row = tile_ids(pack, tile)
                wanted += [row[:, :LANES], row[:, LANES:]]
        wanted = jnp.concatenate(wanted, axis=0)
        picked[...] = jnp.zeros_like(picked)
        mine[...] = jnp.zeros_like(mine)
        count = jnp.sum(bad).astype(jnp.int32)

        def rescue(b, _):
            here = jnp.minimum(count - b * BATCH, BATCH)

            def pick(i, _):
                left = sums[...]
                found = jnp.min(left)
                at = found.astype(jnp.int32)
                chosen[i] = at
                sums[...] = jnp.where(left == found, beyond, left)
                number_of = jnp.sum(jnp.where(place == found, wanted, 0.0))
                mine[pl.ds(i, 1), :] = jnp.full((1, LANES), number_of, jnp.float32)
                inside = lax.rem(at, tokens)
                line = lax.rem(inside, 16)
                start = pl.multiple_of(inside - line, 16)
                for k, pack in enumerate(packs):

                    @pl.when(at // tokens == k)
                    def _(pack=pack):
                        group = pack[pl.ds(start, 16), :].astype(jnp.float32)
                        at_line = lax.broadcasted_iota(jnp.int32, group.shape, 0) == line
                        picked[pl.ds(i, 1), :] = jnp.sum(
                            jnp.where(at_line, group, 0.0), axis=0, keepdims=True
                        )

                return 0

            lax.fori_loop(0, here, pick, 0)
            users = picked[...].astype(jnp.bfloat16)
            ids = mine[...]
            peak = jnp.full((BATCH, LANES), FLOOR, jnp.float32)
            for start in range(0, number, 1024):
                size = min(1024, number - start)
                part = lax.dot_general(
                    users, negs[pl.ds(start, size), :], CONTRACT, preferred_element_type=jnp.float32
                )
                part = part * scale2
                for k in range(size // LANES):
                    row = start // LANES + k
                    other = id_rows[row : row + 1, :].astype(jnp.float32)
                    piece = jnp.where(other == ids, FLOOR, part[:, k * LANES : (k + 1) * LANES])
                    logits[row] = piece
                    peak = jnp.maximum(peak, piece)
            peak = jnp.max(peak, axis=1, keepdims=True)
            amount = jnp.zeros((BATCH, LANES), jnp.float32)
            for row in range(number // LANES):
                piece = logits[row]
                amount = amount + jnp.where(piece > 0.5 * FLOOR, jnp.exp2(piece - peak), 0.0)
            amount = jnp.sum(amount, axis=1, keepdims=True)
            some = amount > 0.0
            value = jnp.where(some, peak + jnp.log2(jnp.where(some, amount, 1.0)), FLOOR)
            values[...] = jnp.broadcast_to(value, (BATCH, LANES))

            def put(i, _):
                at = chosen[i].astype(jnp.float32)
                out[0:lines, :] = jnp.where(place == at, values[pl.ds(i, 1), :], out[0:lines, :])
                return 0

            lax.fori_loop(0, here, put, 0)
            return 0

        lax.fori_loop(0, (count + BATCH - 1) // BATCH, rescue, 0)


def finish_kernel(members, rows, me, gathered, loss_out, totals_out):
    weighted = jnp.zeros((rows, LANES), jnp.float32)
    counted = jnp.zeros((rows, LANES), jnp.float32)
    own = jnp.zeros((rows, LANES), jnp.float32)
    for owner in range(members):
        positive = gathered[owner, members * rows : (members + 1) * rows, :]
        weight = gathered[owner, (members + 1) * rows : (members + 2) * rows, :]
        shares = [
            gathered[k, (owner ^ k) * rows : ((owner ^ k) + 1) * rows, :] for k in range(members)
        ]
        peak = positive
        for share in shares:
            peak = jnp.maximum(peak, share)
        total = jnp.exp2(positive - peak)
        for share in shares:
            total = total + jnp.exp2(share - peak)
        loss = (peak - positive + jnp.log2(total)) * (1.0 / LOG2E)
        loss = jnp.where(weight > 0.0, loss, 0.0)
        weighted = weighted + weight * loss
        counted = counted + weight
        own = jnp.where(me[0] == owner, loss, own)
    loss_out[...] = own
    first = jnp.sum(weighted, axis=0, keepdims=True)
    second = jnp.sum(counted, axis=0, keepdims=True)
    line = lax.broadcasted_iota(jnp.int32, (8, LANES), 0)
    totals_out[...] = jnp.where(line == 0, first, jnp.where(line == 1, second, 0.0))


def call(kernel, shapes, *args, flags=None, cost=None, scratch=(), smem=0, limit=16):
    return pl.pallas_call(
        kernel,
        out_shape=shapes,
        in_specs=[SMEM] * smem + [VMEM] * (len(args) - smem),
        out_specs=jax.tree.map(lambda _: VMEM, shapes),
        scratch_shapes=list(scratch),
        compiler_params=pltpu.CompilerParams(vmem_limit_bytes=limit * 2**20, flags=flags),
        cost_estimate=cost,
    )(*args)


def exchanged(value, axis, size, mask):
    return lax.ppermute(value, axis, [(i, i ^ mask) for i in range(size)])


def shards(
    dp,
    members,
    user_embed,
    positive_embed,
    positive_ids,
    token_weights,
    offsets,
    negative_embed,
    negative_ids,
):
    tokens, width = user_embed.shape
    number = negative_embed.shape[0]
    rows = tokens // LANES
    scale2 = 3.0 / math.sqrt(width) * LOG2E
    me = lax.axis_index("neg").reshape(1).astype(jnp.int32)
    id_rows = negative_ids.reshape(number // LANES, LANES)
    f32 = lambda *shape: jax.ShapeDtypeStruct(shape, jnp.float32)

    def cost(count):
        return pl.CostEstimate(
            flops=2 * count * tokens * number * width,
            bytes_accessed=number * width * 2,
            transcendentals=count * tokens * number,
        )

    pack = call(
        pack_kernel,
        jax.ShapeDtypeStruct((tokens + ID_ROWS, width), user_embed.dtype),
        user_embed,
        positive_ids.reshape(rows, LANES),
        cost=cost(1),
    )
    packs = [pack, exchanged(pack, "neg", members, 1)]
    for mask in [2**k for k in range(1, members.bit_length() - 1)]:
        packs += [exchanged(pack, "neg", members, mask)] + [None] * (mask - 1)
    side = call(
        functools.partial(side_kernel, scale2),
        f32(2 * rows, LANES),
        me,
        offsets,
        pack,
        positive_embed,
        token_weights.reshape(rows, LANES),
        smem=2,
        cost=cost(1),
    )
    own, side = lax.optimization_barrier((pack, side))
    early = [
        call(
            functools.partial(sums_kernel, scale2, 2),
            f32(2 * rows, LANES),
            own,
            packs[1],
            negative_embed,
            id_rows,
            cost=cost(2),
        )
    ]
    for mask in range(2, members):
        if packs[mask] is None:
            low = mask & -mask
            source, early[0] = lax.optimization_barrier((packs[mask ^ low], early[0]))
            packs[mask] = exchanged(source, "neg", members, low)
    for mask in range(2, members - 1):
        early.append(
            call(
                functools.partial(sums_kernel, scale2, 1),
                f32(rows, LANES),
                packs[mask],
                negative_embed,
                id_rows,
                cost=cost(1),
            )
        )
    lines = members * rows
    payload = call(
        functools.partial(last_kernel, scale2, members),
        f32(lines + 2 * rows, LANES),
        *packs,
        negative_embed,
        id_rows,
        *early,
        side,
        cost=cost(1),
        scratch=[
            pltpu.VMEM((lines, LANES), jnp.float32),
            pltpu.SMEM((BATCH,), jnp.int32),
            pltpu.VMEM((BATCH, width), jnp.float32),
            pltpu.VMEM((BATCH, LANES), jnp.float32),
            pltpu.VMEM((number // LANES, BATCH, LANES), jnp.float32),
            pltpu.VMEM((BATCH, LANES), jnp.float32),
        ],
    )
    gathered = lax.all_gather(payload, "neg", axis=0)
    loss, totals = call(
        functools.partial(finish_kernel, members, rows),
        (f32(rows, LANES), f32(8, LANES)),
        me,
        gathered,
        smem=1,
    )
    mask = 1
    while mask < dp:
        totals = totals + exchanged(totals, "dp", dp, mask)
        mask *= 2
    mean = jnp.sum(totals[0]) / jnp.sum(totals[1])
    return (loss.reshape(tokens), mean)


def solution(mesh):
    dp, members = mesh.shape["dp"], mesh.shape["neg"]
    in_specs = (
        P(("dp", "neg"), None),
        P(("dp", "neg"), None),
        P(("dp", "neg")),
        P(("dp", "neg")),
        P("dp", None),
        P("neg", None),
        P("neg"),
    )
    out_specs = (P(("dp", "neg")), P())
    return jax.shard_map(
        functools.partial(shards, dp, members),
        mesh=mesh,
        in_specs=in_specs,
        out_specs=out_specs,
        check_vma=False,
    )
```

```python
import functools
import math

import jax
import jax.numpy as jnp
from jax import lax
from jax.experimental import pallas as pl
from jax.experimental.pallas import tpu as pltpu
from jax.sharding import PartitionSpec as P

LANES = 128
TILE = 256
BLOCK = 512
ID_ROWS = 16
BATCH = 16
LOG2E = math.log2(math.e)
FLOOR = -1e30
HIGHEST = 2.0**126
LOWEST = 2.0**-90
CONTRACT = (((1,), (1,)), ((), ()))
VMEM = pl.BlockSpec(memory_space=pltpu.VMEM)
HBM = pl.BlockSpec(memory_space=pltpu.HBM)
SMEM = pl.BlockSpec(memory_space=pltpu.SMEM)


def pack_kernel(me, users, places, targets, weights, negative_ids, offsets, *rest):
    out, targets_here, live, id_rows, places_here, weights_here, offsets_here, done = rest
    tokens = users.shape[0]
    tiles = tokens // TILE
    rows = tokens // LANES
    pairs = [
        (places, places_here),
        (users, out.at[pl.ds(0, tokens), :]),
        (weights, weights_here),
        (offsets, offsets_here),
        (negative_ids, id_rows),
        (targets, targets_here),
    ]
    copies = [pltpu.make_async_copy(*pair, done.at[k]) for k, pair in enumerate(pairs)]
    for copy in copies:
        copy.start()
    copies[0].wait()
    ids = places_here[...]
    lines = []
    for digit in (ids & 127, (ids >> 7) & 127, ids >> 14):
        digit = digit.astype(jnp.float32)
        for tile in range(tiles):
            lines.append(
                jnp.concatenate(
                    [digit[2 * tile : 2 * tile + 1], digit[2 * tile + 1 : 2 * tile + 2]], axis=1
                )
            )
    lines.append(jnp.zeros((ID_ROWS - len(lines), TILE), jnp.float32))
    out[tokens:, :] = jnp.concatenate(lines, axis=0).astype(out.dtype)
    copies[2].wait()
    copies[3].wait()
    line = lax.broadcasted_iota(jnp.int32, (rows, LANES), 0)
    lane = lax.broadcasted_iota(jnp.int32, (rows, LANES), 1)
    position = me[0] * tokens + line * LANES + lane
    ends = offsets.shape[1]
    has = position < offsets_here[0, ends - 1]
    for user in range(1, ends):
        has = has & (position + 1 != offsets_here[0, user])
    live[...] = jnp.where(has, weights_here[...], 0).astype(jnp.float32)
    for k in (1, 4, 5):
        copies[k].wait()


def tile_ids(pack, tile):
    tokens = pack.shape[0] - ID_ROWS
    tiles = tokens // TILE
    digits = pack[tokens:, :].astype(jnp.float32)
    rows = [digits[d * tiles + tile : d * tiles + tile + 1] for d in range(3)]
    return rows[0] + 128.0 * rows[1] + 16384.0 * rows[2]


def sum_pack(scale2, pack, negs, id_rows, out, first, arrivals=None):
    tokens = pack.shape[0] - ID_ROWS
    number = negs.shape[0]
    tiles = tokens // TILE
    wanted = [
        jnp.broadcast_to(tile_ids(pack, tile), (8, TILE)).astype(jnp.int32) for tile in range(tiles)
    ]
    totals = [jnp.zeros((8, LANES), jnp.float32) for _ in range(2 * tiles)]
    for start in range(0, number, BLOCK):
        size = min(BLOCK, number - start)
        if arrivals and start in arrivals:
            arrivals[start].wait()
        block = negs[pl.ds(start, size), :]
        others = [
            jnp.broadcast_to(id_rows[row : row + 1, :], (LANES, LANES)).T
            for row in range(start // LANES, (start + size) // LANES)
        ]
        others = jnp.concatenate(others, axis=0).reshape(size // 8, 8, LANES)
        for tile in range(tiles):
            users = pack[tile * TILE : (tile + 1) * TILE, :]
            logit = lax.dot_general(block, users, CONTRACT, preferred_element_type=jnp.float32)
            grown = jnp.exp2(logit * scale2)
            for half in range(2):
                lanes = slice(half * LANES, (half + 1) * LANES)
                part = grown[:, lanes].reshape(size // 8, 8, LANES)
                part = jnp.where(others == wanted[tile][None, :, lanes], 0.0, part)
                totals[2 * tile + half] = totals[2 * tile + half] + part.sum(0)
    for row in range(2 * tiles):
        out[first + row : first + row + 1, :] = jnp.sum(totals[row], axis=0, keepdims=True)


def sums_kernel(scale2, pack, negs, id_rows, out):
    sum_pack(scale2, pack, negs, id_rows, out, 0)


def first_kernel(scale2, pack, other, targets, live, id_rows, far, *rest):
    out, side, negs, arrived = rest
    number = negs.shape[0]
    rows = targets.shape[0] // LANES
    edges = [0, min(2 * BLOCK, number), min(8 * BLOCK, number), number]
    arrivals = {}
    for k, (low, high) in enumerate(zip(edges, edges[1:])):
        if low < high:
            part = pl.ds(low, high - low)
            arrivals[low] = pltpu.make_async_copy(far.at[part, :], negs.at[part, :], arrived.at[k])
            arrivals[low].start()
    side_rows(scale2, pack, targets, live, side)
    sum_pack(scale2, pack, negs, id_rows, out, 0, arrivals)
    sum_pack(scale2, other, negs, id_rows, out, rows)


def side_rows(scale2, pack, targets, live, out):
    tokens = targets.shape[0]
    rows = tokens // LANES
    product = pack[0:tokens, :].astype(jnp.float32) * targets[...].astype(jnp.float32)
    high = product.astype(jnp.bfloat16)
    low = (product - high.astype(jnp.float32)).astype(jnp.bfloat16)
    ones = jnp.ones((16, product.shape[1]), jnp.bfloat16)
    positive = lax.dot_general(
        ones, high, CONTRACT, preferred_element_type=jnp.float32
    ) + lax.dot_general(ones, low, CONTRACT, preferred_element_type=jnp.float32)
    positive = positive * scale2
    for row in range(rows):
        out[row : row + 1, :] = positive[0:1, row * LANES : (row + 1) * LANES]
    out[rows:, :] = live[...]


def last_kernel(scale2, members, *refs):
    packs = refs[:members]
    negs, id_rows, *rest = refs[members:]
    early, side, out, sums, chosen, picked, mine, logits, values = (
        rest[: members - 2],
        *rest[members - 2 :],
    )
    tokens = packs[0].shape[0] - ID_ROWS
    number = negs.shape[0]
    rows = tokens // LANES
    lines = members * rows
    first = 0
    for share in early:
        sums[first : first + share.shape[0], :] = share[...]
        first += share.shape[0]
    sum_pack(scale2, packs[-1], negs, id_rows, sums, first)
    total = sums[...]
    good = (total < HIGHEST) & (total > LOWEST)
    out[0:lines, :] = jnp.log2(jnp.where(good, total, 1.0))
    out[lines:, :] = side[...]
    bad = jnp.where(good, 0.0, 1.0)

    @pl.when(jnp.max(bad) > 0.0)
    def _():
        place = lax.broadcasted_iota(jnp.int32, (lines, LANES), 0) * LANES
        place = (place + lax.broadcasted_iota(jnp.int32, (lines, LANES), 1)).astype(jnp.float32)
        beyond = float(lines * LANES)
        sums[...] = jnp.where(good, beyond, place)
        wanted = []
        for pack in packs:
            for tile in range(tokens // TILE):
                row = tile_ids(pack, tile)
                wanted += [row[:, :LANES], row[:, LANES:]]
        wanted = jnp.concatenate(wanted, axis=0)
        picked[...] = jnp.zeros_like(picked)
        mine[...] = jnp.zeros_like(mine)
        count = jnp.sum(bad).astype(jnp.int32)

        def rescue(b, _):
            here = jnp.minimum(count - b * BATCH, BATCH)

            def pick(i, _):
                left = sums[...]
                found = jnp.min(left)
                at = found.astype(jnp.int32)
                chosen[i] = at
                sums[...] = jnp.where(left == found, beyond, left)
                number_of = jnp.sum(jnp.where(place == found, wanted, 0.0))
                mine[pl.ds(i, 1), :] = jnp.full((1, LANES), number_of, jnp.float32)
                inside = lax.rem(at, tokens)
                line = lax.rem(inside, 16)
                start = pl.multiple_of(inside - line, 16)
                for k, pack in enumerate(packs):

                    @pl.when(at // tokens == k)
                    def _(pack=pack):
                        group = pack[pl.ds(start, 16), :].astype(jnp.float32)
                        at_line = lax.broadcasted_iota(jnp.int32, group.shape, 0) == line
                        picked[pl.ds(i, 1), :] = jnp.sum(
                            jnp.where(at_line, group, 0.0), axis=0, keepdims=True
                        )

                return 0

            lax.fori_loop(0, here, pick, 0)
            users = picked[...].astype(jnp.bfloat16)
            ids = mine[...]
            peak = jnp.full((BATCH, LANES), FLOOR, jnp.float32)
            for start in range(0, number, 1024):
                size = min(1024, number - start)
                part = lax.dot_general(
                    users, negs[pl.ds(start, size), :], CONTRACT, preferred_element_type=jnp.float32
                )
                part = part * scale2
                for k in range(size // LANES):
                    row = start // LANES + k
                    other = id_rows[row : row + 1, :].astype(jnp.float32)
                    piece = jnp.where(other == ids, FLOOR, part[:, k * LANES : (k + 1) * LANES])
                    logits[row] = piece
                    peak = jnp.maximum(peak, piece)
            peak = jnp.max(peak, axis=1, keepdims=True)
            amount = jnp.zeros((BATCH, LANES), jnp.float32)
            for row in range(number // LANES):
                piece = logits[row]
                amount = amount + jnp.where(piece > 0.5 * FLOOR, jnp.exp2(piece - peak), 0.0)
            amount = jnp.sum(amount, axis=1, keepdims=True)
            some = amount > 0.0
            value = jnp.where(some, peak + jnp.log2(jnp.where(some, amount, 1.0)), FLOOR)
            values[...] = jnp.broadcast_to(value, (BATCH, LANES))

            def put(i, _):
                at = chosen[i].astype(jnp.float32)
                out[0:lines, :] = jnp.where(place == at, values[pl.ds(i, 1), :], out[0:lines, :])
                return 0

            lax.fori_loop(0, here, put, 0)
            return 0

        lax.fori_loop(0, (count + BATCH - 1) // BATCH, rescue, 0)


def finish_kernel(members, rows, me, gathered, loss_out, totals_out):
    weighted = jnp.zeros((rows, LANES), jnp.float32)
    counted = jnp.zeros((rows, LANES), jnp.float32)
    own = jnp.zeros((rows, LANES), jnp.float32)
    for owner in range(members):
        positive = gathered[owner, members * rows : (members + 1) * rows, :]
        weight = gathered[owner, (members + 1) * rows : (members + 2) * rows, :]
        shares = [
            gathered[k, (owner ^ k) * rows : ((owner ^ k) + 1) * rows, :] for k in range(members)
        ]
        peak = positive
        for share in shares:
            peak = jnp.maximum(peak, share)
        total = jnp.exp2(positive - peak)
        for share in shares:
            total = total + jnp.exp2(share - peak)
        loss = (peak - positive + jnp.log2(total)) * (1.0 / LOG2E)
        loss = jnp.where(weight > 0.0, loss, 0.0)
        weighted = weighted + weight * loss
        counted = counted + weight
        own = jnp.where(me[0] == owner, loss, own)
    loss_out[...] = own
    first = jnp.sum(weighted, axis=0, keepdims=True)
    second = jnp.sum(counted, axis=0, keepdims=True)
    line = lax.broadcasted_iota(jnp.int32, (8, LANES), 0)
    totals_out[...] = jnp.where(line == 0, first, jnp.where(line == 1, second, 0.0))


def mean_kernel(totals, received, out):
    totals = totals[...] + received[...]
    weighted = jnp.sum(totals[0:1], axis=1, keepdims=True)
    out[...] = weighted / jnp.sum(totals[1:2], axis=1, keepdims=True)


def call(kernel, shapes, *args, cost=None, scratch=(), smem=0, far=(), limit=16):
    specs = [SMEM] * smem + [VMEM] * (len(args) - smem)
    args = list(args)
    for place in far:
        specs[place] = HBM
        args[place] = pltpu.with_memory_space_constraint(args[place], pltpu.HBM)
    return pl.pallas_call(
        kernel,
        out_shape=shapes,
        in_specs=specs,
        out_specs=jax.tree.map(lambda _: VMEM, shapes),
        scratch_shapes=list(scratch),
        compiler_params=pltpu.CompilerParams(vmem_limit_bytes=limit * 2**20),
        cost_estimate=cost,
    )(*args)


def exchanged(value, axis, size, mask):
    return lax.ppermute(value, axis, [(i, i ^ mask) for i in range(size)])


def shards(
    dp,
    members,
    user_embed,
    positive_embed,
    positive_ids,
    token_weights,
    offsets,
    negative_embed,
    negative_ids,
):
    tokens, width = user_embed.shape
    number = negative_embed.shape[0]
    rows = tokens // LANES
    scale2 = 3.0 / math.sqrt(width) * LOG2E
    me = lax.axis_index("neg").reshape(1).astype(jnp.int32)
    id_rows = negative_ids.reshape(number // LANES, LANES)
    f32 = lambda *shape: jax.ShapeDtypeStruct(shape, jnp.float32)

    def cost(count):
        return pl.CostEstimate(
            flops=2 * count * tokens * number * width,
            bytes_accessed=number * width * 2,
            transcendentals=count * tokens * number,
        )

    like = lambda array: jax.ShapeDtypeStruct(array.shape, array.dtype)
    pack, targets, live, id_rows = call(
        pack_kernel,
        (
            jax.ShapeDtypeStruct((tokens + ID_ROWS, width), user_embed.dtype),
            like(positive_embed),
            f32(rows, LANES),
            like(id_rows),
        ),
        me,
        user_embed,
        positive_ids.reshape(rows, LANES),
        positive_embed,
        token_weights.reshape(rows, LANES),
        id_rows,
        offsets,
        smem=1,
        far=range(1, 7),
        scratch=[
            pltpu.VMEM((rows, LANES), jnp.int32),
            pltpu.VMEM((rows, LANES), jnp.int32),
            pltpu.SMEM(offsets.shape, jnp.int32),
            pltpu.SemaphoreType.DMA((6,)),
        ],
        limit=4,
    )
    packs = [pack, exchanged(pack, "neg", members, 1)]
    for mask in [2**k for k in range(1, members.bit_length() - 1)]:
        packs += [exchanged(pack, "neg", members, mask)] + [None] * (mask - 1)
    shares, side, negatives = call(
        functools.partial(first_kernel, scale2),
        (
            f32(2 * rows, LANES),
            f32(2 * rows, LANES),
            like(negative_embed),
        ),
        *packs[:2],
        targets,
        live,
        id_rows,
        negative_embed,
        far=(5,),
        cost=cost(2),
        scratch=[pltpu.SemaphoreType.DMA((3,))],
    )
    early = [shares]
    for mask in range(2, members):
        if packs[mask] is None:
            low = mask & -mask
            source, early[0] = lax.optimization_barrier((packs[mask ^ low], early[0]))
            packs[mask] = exchanged(source, "neg", members, low)
    for mask in range(2, members - 1):
        early.append(
            call(
                functools.partial(sums_kernel, scale2),
                f32(rows, LANES),
                packs[mask],
                negatives,
                id_rows,
                cost=cost(1),
            )
        )
    lines = members * rows
    payload = call(
        functools.partial(last_kernel, scale2, members),
        f32(lines + 2 * rows, LANES),
        *packs,
        negatives,
        id_rows,
        *early,
        side,
        cost=cost(1),
        scratch=[
            pltpu.VMEM((lines, LANES), jnp.float32),
            pltpu.SMEM((BATCH,), jnp.int32),
            pltpu.VMEM((BATCH, width), jnp.float32),
            pltpu.VMEM((BATCH, LANES), jnp.float32),
            pltpu.VMEM((number // LANES, BATCH, LANES), jnp.float32),
            pltpu.VMEM((BATCH, LANES), jnp.float32),
        ],
    )
    gathered = lax.all_gather(payload, "neg", axis=0)
    loss, totals = call(
        functools.partial(finish_kernel, members, rows),
        (f32(rows, LANES), f32(8, LANES)),
        me,
        gathered,
        smem=1,
        limit=2,
    )
    mask = 1
    while mask < dp:
        received = exchanged(totals, "dp", dp, mask)
        mask *= 2
        if mask < dp:
            totals = totals + received
    mean = call(mean_kernel, f32(1, 1), totals, received, limit=1)
    return (loss.reshape(tokens), mean.reshape(()))


def solution(mesh):
    dp, members = mesh.shape["dp"], mesh.shape["neg"]
    in_specs = (
        P(("dp", "neg"), None),
        P(("dp", "neg"), None),
        P(("dp", "neg")),
        P(("dp", "neg")),
        P("dp", None),
        P("neg", None),
        P("neg"),
    )
    out_specs = (P(("dp", "neg")), P())
    return jax.shard_map(
        functools.partial(shards, dp, members),
        mesh=mesh,
        in_specs=in_specs,
        out_specs=out_specs,
        check_vma=False,
    )
```

```python
import functools
import math

import jax
import jax.numpy as jnp
from jax import lax
from jax.experimental import pallas as pl
from jax.experimental.pallas import tpu as pltpu
from jax.sharding import PartitionSpec as P

LANES = 128
TILE = 256
BLOCK = 2048
ID_ROWS = 16
BATCH = 16
LOG2E = math.log2(math.e)
FLOOR = -1e30
HIGHEST = 2.0**126
LOWEST = 2.0**-90
CONTRACT = (((1,), (1,)), ((), ()))
VMEM = pl.BlockSpec(memory_space=pltpu.VMEM)
HBM = pl.BlockSpec(memory_space=pltpu.HBM)
SMEM = pl.BlockSpec(memory_space=pltpu.SMEM)
def pack_kernel(me, users, places, targets, weights, negative_ids, offsets, *rest):
    out, targets_here, live, id_rows, places_here, weights_here, offsets_here, done = rest
    tokens = users.shape[0]
    tiles = tokens // TILE
    rows = tokens // LANES
    pairs = [
        (places, places_here),
        (users, out.at[pl.ds(0, tokens), :]),
        (weights, weights_here),
        (offsets, offsets_here),
        (negative_ids, id_rows),
        (targets, targets_here),
    ]
    copies = [pltpu.make_async_copy(*pair, done.at[k]) for k, pair in enumerate(pairs)]
    for copy in copies:
        copy.start()
    copies[0].wait()
    ids = places_here[...]
    lines = []
    for digit in (ids & 127, (ids >> 7) & 127, ids >> 14):
        digit = digit.astype(jnp.float32)
        for tile in range(tiles):
            lines.append(
                jnp.concatenate(
                    [digit[2 * tile : 2 * tile + 1], digit[2 * tile + 1 : 2 * tile + 2]], axis=1
                )
            )
    lines.append(jnp.zeros((ID_ROWS - len(lines), TILE), jnp.float32))
    out[tokens:, :] = jnp.concatenate(lines, axis=0).astype(out.dtype)
    copies[2].wait()
    copies[3].wait()
    line = lax.broadcasted_iota(jnp.int32, (rows, LANES), 0)
    lane = lax.broadcasted_iota(jnp.int32, (rows, LANES), 1)
    position = me[0] * tokens + line * LANES + lane
    ends = offsets.shape[1]
    has = position < offsets_here[0, ends - 1]
    for user in range(1, ends):
        has = has & (position + 1 != offsets_here[0, user])
    live[...] = jnp.where(has, weights_here[...], 0).astype(jnp.float32)
    for k in (1, 4, 5):
        copies[k].wait()


def tile_ids(pack, tile):
    tokens = pack.shape[0] - ID_ROWS
    tiles = tokens // TILE
    digits = pack[tokens:, :].astype(jnp.float32)
    rows = [digits[d * tiles + tile : d * tiles + tile + 1] for d in range(3)]
    return rows[0] + 128.0 * rows[1] + 16384.0 * rows[2]


def sum_pack(scale2, pack, negs, id_rows, out, first, arrivals=None):
    tokens = pack.shape[0] - ID_ROWS
    number = negs.shape[0]
    tiles = tokens // TILE
    wanted = [
        jnp.broadcast_to(tile_ids(pack, tile), (8, TILE)).astype(jnp.int32) for tile in range(tiles)
    ]
    totals = [jnp.zeros((8, LANES), jnp.float32) for _ in range(2 * tiles)]
    cuts = sorted({*range(0, number, BLOCK), *(arrivals or ()), number})
    for start, stop in zip(cuts, cuts[1:]):
        size = stop - start
        if arrivals and start in arrivals:
            arrivals[start].wait()
        block = negs[pl.ds(start, size), :]
        others = [
            jnp.broadcast_to(id_rows[row : row + 1, :], (LANES, LANES)).T
            for row in range(start // LANES, stop // LANES)
        ]
        others = jnp.concatenate(others, axis=0).reshape(size // 8, 8, LANES)
        for tile in range(tiles):
            users = pack[tile * TILE : (tile + 1) * TILE, :]
            logit = lax.dot_general(block, users, CONTRACT, preferred_element_type=jnp.float32)
            grown = jnp.exp2(logit * scale2)
            for half in range(2):
                lanes = slice(half * LANES, (half + 1) * LANES)
                part = grown[:, lanes].reshape(size // 8, 8, LANES)
                part = jnp.where(others == wanted[tile][None, :, lanes], 0.0, part)
                totals[2 * tile + half] = totals[2 * tile + half] + part.sum(0)
    for row in range(2 * tiles):
        out[first + row : first + row + 1, :] = jnp.sum(totals[row], axis=0, keepdims=True)


def sums_kernel(scale2, pack, negs, id_rows, out):
    sum_pack(scale2, pack, negs, id_rows, out, 0)


def first_kernel(scale2, pack, other, targets, live, id_rows, far, *rest):
    out, side, negs, arrived = rest
    number = negs.shape[0]
    rows = targets.shape[0] // LANES
    edges = [0, min(BLOCK // 4, number), min(BLOCK, number), number]
    arrivals = {}
    for k, (low, high) in enumerate(zip(edges, edges[1:])):
        if low < high:
            part = pl.ds(low, high - low)
            arrivals[low] = pltpu.make_async_copy(far.at[part, :], negs.at[part, :], arrived.at[k])
            arrivals[low].start()
    side_rows(scale2, pack, targets, live, side)
    sum_pack(scale2, pack, negs, id_rows, out, 0, arrivals)
    sum_pack(scale2, other, negs, id_rows, out, rows)


def side_rows(scale2, pack, targets, live, out):
    tokens = targets.shape[0]
    rows = tokens // LANES
    product = pack[0:tokens, :].astype(jnp.float32) * targets[...].astype(jnp.float32)
    high = product.astype(jnp.bfloat16)
    low = (product - high.astype(jnp.float32)).astype(jnp.bfloat16)
    ones = jnp.ones((16, product.shape[1]), jnp.bfloat16)
    positive = lax.dot_general(
        ones, high, CONTRACT, preferred_element_type=jnp.float32
    ) + lax.dot_general(ones, low, CONTRACT, preferred_element_type=jnp.float32)
    positive = positive * scale2
    for row in range(rows):
        out[row : row + 1, :] = positive[0:1, row * LANES : (row + 1) * LANES]
    out[rows:, :] = live[...]


def last_kernel(scale2, members, *refs):
    packs = refs[:members]
    negs, id_rows, *rest = refs[members:]
    early, side, out, sums, chosen, picked, mine, logits, values, wanted_ref = (
        rest[: members - 2],
        *rest[members - 2 :],
    )
    tokens = packs[0].shape[0] - ID_ROWS
    number = negs.shape[0]
    rows = tokens // LANES
    lines = members * rows
    first = 0
    for share in early:
        sums[first : first + share.shape[0], :] = share[...]
        first += share.shape[0]
    sum_pack(scale2, packs[-1], negs, id_rows, sums, first)
    total = sums[...]
    good = (total < HIGHEST) & (total > LOWEST)
    out[0:lines, :] = jnp.log2(jnp.where(good, total, 1.0))
    out[lines:, :] = side[...]
    bad = jnp.where(good, 0.0, 1.0)

    count = jnp.sum(bad).astype(jnp.int32)

    @pl.when(count > 0)
    def _():
        place = lax.broadcasted_iota(jnp.int32, (lines, LANES), 0) * LANES
        place = (place + lax.broadcasted_iota(jnp.int32, (lines, LANES), 1)).astype(jnp.float32)
        beyond = float(lines * LANES)
        sums[...] = jnp.where(good, beyond, place)
        wanted = []
        for pack in packs:
            for tile in range(tokens // TILE):
                row = tile_ids(pack, tile)
                wanted += [row[:, :LANES], row[:, LANES:]]
        wanted_ref[...] = jnp.concatenate(wanted, axis=0)
        picked[...] = jnp.zeros_like(picked)
        mine[...] = jnp.zeros_like(mine)

        def rescue(b, _):
            here = jnp.minimum(count - b * BATCH, BATCH)

            def pick(i, _):
                left = sums[...]
                found = jnp.min(left)
                at = found.astype(jnp.int32)
                chosen[i] = at
                sums[...] = jnp.where(left == found, beyond, left)
                near = wanted_ref[pl.ds(at // LANES, 1), :]
                lane = lax.broadcasted_iota(jnp.int32, (1, LANES), 1)
                near = jnp.where(lane == lax.rem(at, LANES), near, 0.0)
                near = jnp.sum(near, axis=1, keepdims=True)
                mine[pl.ds(i, 1), :] = jnp.broadcast_to(near, (1, LANES))
                inside = lax.rem(at, tokens)
                line = lax.rem(inside, 16)
                start = pl.multiple_of(inside - line, 16)
                for k, pack in enumerate(packs):

                    @pl.when(at // tokens == k)
                    def _(pack=pack):
                        group = pack[pl.ds(start, 16), :].astype(jnp.float32)
                        at_line = lax.broadcasted_iota(jnp.int32, group.shape, 0) == line
                        picked[pl.ds(i, 1), :] = jnp.sum(
                            jnp.where(at_line, group, 0.0), axis=0, keepdims=True
                        )

                return 0

            lax.fori_loop(0, here, pick, 0)
            users = picked[...].astype(jnp.bfloat16)
            ids = mine[...]
            peak = jnp.full((BATCH, LANES), FLOOR, jnp.float32)
            for start in range(0, number, 1024):
                size = min(1024, number - start)
                part = lax.dot_general(
                    users, negs[pl.ds(start, size), :], CONTRACT, preferred_element_type=jnp.float32
                )
                part = part * scale2
                for k in range(size // LANES):
                    row = start // LANES + k
                    other = id_rows[row : row + 1, :].astype(jnp.float32)
                    piece = jnp.where(other == ids, FLOOR, part[:, k * LANES : (k + 1) * LANES])
                    logits[row] = piece
                    peak = jnp.maximum(peak, piece)
            peak = jnp.max(peak, axis=1, keepdims=True)
            amount = jnp.zeros((BATCH, LANES), jnp.float32)
            for row in range(number // LANES):
                piece = logits[row]
                amount = amount + jnp.where(piece > 0.5 * FLOOR, jnp.exp2(piece - peak), 0.0)
            amount = jnp.sum(amount, axis=1, keepdims=True)
            some = amount > 0.0
            value = jnp.where(some, peak + jnp.log2(jnp.where(some, amount, 1.0)), FLOOR)
            values[...] = jnp.broadcast_to(value, (BATCH, LANES))

            def put(i, _):
                at = chosen[i].astype(jnp.float32)
                out[0:lines, :] = jnp.where(place == at, values[pl.ds(i, 1), :], out[0:lines, :])
                return 0

            lax.fori_loop(0, here, put, 0)
            return 0

        lax.fori_loop(0, (count + BATCH - 1) // BATCH, rescue, 0)


def finish_kernel(members, rows, me, gathered, loss_out, totals_out):
    weighted = jnp.zeros((rows, LANES), jnp.float32)
    counted = jnp.zeros((rows, LANES), jnp.float32)
    own = jnp.zeros((rows, LANES), jnp.float32)
    for owner in range(members):
        positive = gathered[owner, members * rows : (members + 1) * rows, :]
        weight = gathered[owner, (members + 1) * rows : (members + 2) * rows, :]
        shares = [
            gathered[k, (owner ^ k) * rows : ((owner ^ k) + 1) * rows, :] for k in range(members)
        ]
        peak = positive
        for share in shares:
            peak = jnp.maximum(peak, share)
        total = jnp.exp2(positive - peak)
        for share in shares:
            total = total + jnp.exp2(share - peak)
        loss = (peak - positive + jnp.log2(total)) * (1.0 / LOG2E)
        loss = jnp.where(weight > 0.0, loss, 0.0)
        weighted = weighted + weight * loss
        counted = counted + weight
        own = jnp.where(me[0] == owner, loss, own)
    loss_out[...] = own
    first = jnp.sum(weighted, axis=0, keepdims=True)
    second = jnp.sum(counted, axis=0, keepdims=True)
    line = lax.broadcasted_iota(jnp.int32, (8, LANES), 0)
    totals_out[...] = jnp.where(line == 0, first, jnp.where(line == 1, second, 0.0))


def mean_kernel(totals, received, out):
    totals = totals[...] + received[...]
    weighted = jnp.sum(totals[0:1], axis=1, keepdims=True)
    out[...] = weighted / jnp.sum(totals[1:2], axis=1, keepdims=True)


def call(kernel, shapes, *args, cost=None, scratch=(), smem=0, far=(), limit=16):
    specs = [SMEM] * smem + [VMEM] * (len(args) - smem)
    args = list(args)
    for place in far:
        specs[place] = HBM
        args[place] = pltpu.with_memory_space_constraint(args[place], pltpu.HBM)
    return pl.pallas_call(
        kernel,
        out_shape=shapes,
        in_specs=specs,
        out_specs=jax.tree.map(lambda _: VMEM, shapes),
        scratch_shapes=list(scratch),
        compiler_params=pltpu.CompilerParams(vmem_limit_bytes=limit * 2**20),
        cost_estimate=cost,
    )(*args)


def exchanged(value, axis, size, mask):
    return lax.ppermute(value, axis, [(i, i ^ mask) for i in range(size)])


def shards(
    dp,
    members,
    user_embed,
    positive_embed,
    positive_ids,
    token_weights,
    offsets,
    negative_embed,
    negative_ids,
):
    tokens, width = user_embed.shape
    number = negative_embed.shape[0]
    rows = tokens // LANES
    scale2 = 3.0 / math.sqrt(width) * LOG2E
    me = lax.axis_index("neg").reshape(1).astype(jnp.int32)
    id_rows = negative_ids.reshape(number // LANES, LANES)
    f32 = lambda *shape: jax.ShapeDtypeStruct(shape, jnp.float32)

    def cost(count):
        return pl.CostEstimate(
            flops=2 * count * tokens * number * width,
            bytes_accessed=number * width * 2,
            transcendentals=count * tokens * number,
        )

    like = lambda array: jax.ShapeDtypeStruct(array.shape, array.dtype)
    pack, targets, live, id_rows = call(
        pack_kernel,
        (
            jax.ShapeDtypeStruct((tokens + ID_ROWS, width), user_embed.dtype),
            like(positive_embed),
            f32(rows, LANES),
            like(id_rows),
        ),
        me,
        user_embed,
        positive_ids.reshape(rows, LANES),
        positive_embed,
        token_weights.reshape(rows, LANES),
        id_rows,
        offsets,
        smem=1,
        far=range(1, 7),
        scratch=[
            pltpu.VMEM((rows, LANES), jnp.int32),
            pltpu.VMEM((rows, LANES), jnp.int32),
            pltpu.SMEM(offsets.shape, jnp.int32),
            pltpu.SemaphoreType.DMA((6,)),
        ],
        limit=4,
    )
    packs = [pack, exchanged(pack, "neg", members, 1)]
    for mask in [2**k for k in range(1, members.bit_length() - 1)]:
        packs += [exchanged(pack, "neg", members, mask)] + [None] * (mask - 1)
    shares, side, negatives = call(
        functools.partial(first_kernel, scale2),
        (
            f32(2 * rows, LANES),
            f32(2 * rows, LANES),
            like(negative_embed),
        ),
        *packs[:2],
        targets,
        live,
        id_rows,
        negative_embed,
        far=(5,),
        cost=cost(2),
        scratch=[pltpu.SemaphoreType.DMA((3,))],
    )
    early = [shares]
    for mask in range(2, members):
        if packs[mask] is None:
            low = mask & -mask
            source, early[0] = lax.optimization_barrier((packs[mask ^ low], early[0]))
            packs[mask] = exchanged(source, "neg", members, low)
    for mask in range(2, members - 1):
        early.append(
            call(
                functools.partial(sums_kernel, scale2),
                f32(rows, LANES),
                packs[mask],
                negatives,
                id_rows,
                cost=cost(1),
                    )
        )
    lines = members * rows
    payload = call(
        functools.partial(last_kernel, scale2, members),
        f32(lines + 2 * rows, LANES),
        *packs,
        negatives,
        id_rows,
        *early,
        side,
        cost=cost(1),
        scratch=[
            pltpu.VMEM((lines, LANES), jnp.float32),
            pltpu.SMEM((BATCH,), jnp.int32),
            pltpu.VMEM((BATCH, width), jnp.float32),
            pltpu.VMEM((BATCH, LANES), jnp.float32),
            pltpu.VMEM((number // LANES, BATCH, LANES), jnp.float32),
            pltpu.VMEM((BATCH, LANES), jnp.float32),
            pltpu.VMEM((lines, LANES), jnp.float32),
        ],
    )
    gathered = lax.all_gather(payload, "neg", axis=0)
    loss, totals = call(
        functools.partial(finish_kernel, members, rows),
        (f32(rows, LANES), f32(8, LANES)),
        me,
        gathered,
        smem=1,
        limit=2,
    )
    mask = 1
    while mask < dp:
        received = exchanged(totals, "dp", dp, mask)
        mask *= 2
        if mask < dp:
            totals = totals + received
    mean = call(mean_kernel, f32(1, 1), totals, received, limit=1)
    return (loss.reshape(tokens), mean.reshape(()))


def solution(mesh):
    dp, members = mesh.shape["dp"], mesh.shape["neg"]
    in_specs = (
        P(("dp", "neg"), None),
        P(("dp", "neg"), None),
        P(("dp", "neg")),
        P(("dp", "neg")),
        P("dp", None),
        P("neg", None),
        P("neg"),
    )
    out_specs = (P(("dp", "neg")), P())
    return jax.shard_map(
        functools.partial(shards, dp, members),
        mesh=mesh,
        in_specs=in_specs,
        out_specs=out_specs,
        check_vma=False,
    )
```

```python
import functools
import math

import jax
import jax.numpy as jnp
from jax import lax
from jax.experimental import pallas as pl
from jax.experimental.pallas import tpu as pltpu
from jax.sharding import PartitionSpec as P


LANES = 128
TILE = 256
BLOCK = 2048
ID_ROWS = 16
BATCH = 16
LOG2E = math.log2(math.e)
FLOOR = -1e30
HIGHEST = 2.0**126
LOWEST = 2.0**-90
CONTRACT = (((1,), (1,)), ((), ()))
VMEM = pl.BlockSpec(memory_space=pltpu.VMEM)
HBM = pl.BlockSpec(memory_space=pltpu.HBM)
SMEM = pl.BlockSpec(memory_space=pltpu.SMEM)


def pack_kernel(me, users, places, targets, weights, negative_ids, offsets, *rest):
    out, targets_here, live, id_rows, places_here, weights_here, offsets_here, done = rest
    tokens = users.shape[0]
    tiles = tokens // TILE
    rows = tokens // LANES
    pairs = [
        (places, places_here),
        (users, out.at[pl.ds(0, tokens), :]),
        (weights, weights_here),
        (offsets, offsets_here),
        (negative_ids, id_rows),
        (targets, targets_here),
    ]
    copies = [pltpu.make_async_copy(*pair, done.at[k]) for k, pair in enumerate(pairs)]
    for copy in copies:
        copy.start()
    copies[0].wait()
    ids = places_here[...]
    lines = []
    for digit in (ids & 127, (ids >> 7) & 127, ids >> 14):
        digit = digit.astype(jnp.float32)
        for tile in range(tiles):
            lines.append(
                jnp.concatenate(
                    [digit[2 * tile : 2 * tile + 1], digit[2 * tile + 1 : 2 * tile + 2]], axis=1
                )
            )
    lines.append(jnp.zeros((ID_ROWS - len(lines), TILE), jnp.float32))
    out[tokens:, :] = jnp.concatenate(lines, axis=0).astype(out.dtype)
    copies[2].wait()
    copies[3].wait()
    line = lax.broadcasted_iota(jnp.int32, (rows, LANES), 0)
    lane = lax.broadcasted_iota(jnp.int32, (rows, LANES), 1)
    position = me[0] * tokens + line * LANES + lane
    ends = offsets.shape[1]
    has = position < offsets_here[0, ends - 1]
    for user in range(1, ends):
        has = has & (position + 1 != offsets_here[0, user])
    live[...] = jnp.where(has, weights_here[...], 0).astype(jnp.float32)
    for k in (1, 4, 5):
        copies[k].wait()


def tile_ids(pack, tile):
    tokens = pack.shape[0] - ID_ROWS
    tiles = tokens // TILE
    digits = pack[tokens:, :].astype(jnp.float32)
    rows = [digits[d * tiles + tile : d * tiles + tile + 1] for d in range(3)]
    return rows[0] + 128.0 * rows[1] + 16384.0 * rows[2]


def sum_pack(scale2, pack, negs, id_rows, out, first, arrivals=None):
    tokens = pack.shape[0] - ID_ROWS
    number = negs.shape[0]
    tiles = tokens // TILE
    wanted = [
        jnp.broadcast_to(tile_ids(pack, tile), (8, TILE)).astype(jnp.int32) for tile in range(tiles)
    ]
    totals = [jnp.zeros((8, LANES), jnp.float32) for _ in range(2 * tiles)]
    cuts = sorted({*range(0, number, BLOCK), *(arrivals or ()), number})
    for start, stop in zip(cuts, cuts[1:]):
        size = stop - start
        if arrivals and start in arrivals:
            arrivals[start].wait()
        block = negs[pl.ds(start, size), :]
        others = [
            jnp.broadcast_to(id_rows[row : row + 1, :], (LANES, LANES)).T
            for row in range(start // LANES, stop // LANES)
        ]
        others = jnp.concatenate(others, axis=0).reshape(size // 8, 8, LANES)
        for tile in range(tiles):
            users = pack[tile * TILE : (tile + 1) * TILE, :]
            logit = lax.dot_general(block, users, CONTRACT, preferred_element_type=jnp.float32)
            grown = jnp.exp2(logit * scale2)
            for half in range(2):
                lanes = slice(half * LANES, (half + 1) * LANES)
                part = grown[:, lanes].reshape(size // 8, 8, LANES)
                part = jnp.where(others == wanted[tile][None, :, lanes], 0.0, part)
                totals[2 * tile + half] = totals[2 * tile + half] + part.sum(0)
    for row in range(2 * tiles):
        out[first + row : first + row + 1, :] = jnp.sum(totals[row], axis=0, keepdims=True)


def sums_kernel(scale2, pack, negs, id_rows, out):
    sum_pack(scale2, pack, negs, id_rows, out, 0)


def first_kernel(scale2, pack, other, targets, live, id_rows, far, *rest):
    out, side, negs, arrived = rest
    number = negs.shape[0]
    rows = targets.shape[0] // LANES
    edges = [0, min(BLOCK // 4, number), min(BLOCK, number), number]
    arrivals = {}
    for k, (low, high) in enumerate(zip(edges, edges[1:])):
        if low < high:
            part = pl.ds(low, high - low)
            arrivals[low] = pltpu.make_async_copy(far.at[part, :], negs.at[part, :], arrived.at[k])
            arrivals[low].start()
    side_rows(scale2, pack, targets, live, side)
    sum_pack(scale2, pack, negs, id_rows, out, 0, arrivals)
    sum_pack(scale2, other, negs, id_rows, out, rows)


def side_rows(scale2, pack, targets, live, out):
    tokens = targets.shape[0]
    rows = tokens // LANES
    product = pack[0:tokens, :].astype(jnp.float32) * targets[...].astype(jnp.float32)
    high = product.astype(jnp.bfloat16)
    low = (product - high.astype(jnp.float32)).astype(jnp.bfloat16)
    ones = jnp.ones((16, product.shape[1]), jnp.bfloat16)
    positive = lax.dot_general(
        ones, high, CONTRACT, preferred_element_type=jnp.float32
    ) + lax.dot_general(ones, low, CONTRACT, preferred_element_type=jnp.float32)
    positive = positive * scale2
    for row in range(rows):
        out[row : row + 1, :] = positive[0:1, row * LANES : (row + 1) * LANES]
    out[rows:, :] = live[...]


def last_kernel(scale2, members, *refs):
    packs = refs[:members]
    negs, id_rows, *rest = refs[members:]
    early, side, out, sums, chosen, picked, mine, logits, values, wanted_ref = (
        rest[: members - 2],
        *rest[members - 2 :],
    )
    tokens = packs[0].shape[0] - ID_ROWS
    number = negs.shape[0]
    rows = tokens // LANES
    lines = members * rows
    first = 0
    for share in early:
        sums[first : first + share.shape[0], :] = share[...]
        first += share.shape[0]
    sum_pack(scale2, packs[-1], negs, id_rows, sums, first)
    total = sums[...]
    good = (total < HIGHEST) & (total > LOWEST)
    out[0:lines, :] = jnp.log2(jnp.where(good, total, 1.0))
    out[lines:, :] = side[...]
    bad = jnp.where(good, 0.0, 1.0)

    count = jnp.sum(bad).astype(jnp.int32)

    @pl.when(count > 0)
    def _():
        place = lax.broadcasted_iota(jnp.int32, (lines, LANES), 0) * LANES
        place = (place + lax.broadcasted_iota(jnp.int32, (lines, LANES), 1)).astype(jnp.float32)
        beyond = float(lines * LANES)
        sums[...] = jnp.where(good, beyond, place)
        wanted = []
        for pack in packs:
            for tile in range(tokens // TILE):
                row = tile_ids(pack, tile)
                wanted += [row[:, :LANES], row[:, LANES:]]
        wanted_ref[...] = jnp.concatenate(wanted, axis=0)
        picked[...] = jnp.zeros_like(picked)
        mine[...] = jnp.zeros_like(mine)

        def rescue(b, _):
            here = jnp.minimum(count - b * BATCH, BATCH)

            def pick(i, _):
                left = sums[...]
                found = jnp.min(left)
                at = found.astype(jnp.int32)
                chosen[i] = at
                sums[...] = jnp.where(left == found, beyond, left)
                near = wanted_ref[pl.ds(at // LANES, 1), :]
                lane = lax.broadcasted_iota(jnp.int32, (1, LANES), 1)
                near = jnp.where(lane == lax.rem(at, LANES), near, 0.0)
                near = jnp.sum(near, axis=1, keepdims=True)
                mine[pl.ds(i, 1), :] = jnp.broadcast_to(near, (1, LANES))
                inside = lax.rem(at, tokens)
                line = lax.rem(inside, 16)
                start = pl.multiple_of(inside - line, 16)
                for k, pack in enumerate(packs):

                    @pl.when(at // tokens == k)
                    def _(pack=pack):
                        group = pack[pl.ds(start, 16), :].astype(jnp.float32)
                        at_line = lax.broadcasted_iota(jnp.int32, group.shape, 0) == line
                        picked[pl.ds(i, 1), :] = jnp.sum(
                            jnp.where(at_line, group, 0.0), axis=0, keepdims=True
                        )

                return 0

            lax.fori_loop(0, here, pick, 0)
            users = picked[...].astype(jnp.bfloat16)
            ids = mine[...]
            peak = jnp.full((BATCH, LANES), FLOOR, jnp.float32)
            for start in range(0, number, 1024):
                size = min(1024, number - start)
                part = lax.dot_general(
                    users, negs[pl.ds(start, size), :], CONTRACT, preferred_element_type=jnp.float32
                )
                part = part * scale2
                for k in range(size // LANES):
                    row = start // LANES + k
                    other = id_rows[row : row + 1, :].astype(jnp.float32)
                    piece = jnp.where(other == ids, FLOOR, part[:, k * LANES : (k + 1) * LANES])
                    logits[row] = piece
                    peak = jnp.maximum(peak, piece)
            peak = jnp.max(peak, axis=1, keepdims=True)
            amount = jnp.zeros((BATCH, LANES), jnp.float32)
            for row in range(number // LANES):
                piece = logits[row]
                amount = amount + jnp.where(piece > 0.5 * FLOOR, jnp.exp2(piece - peak), 0.0)
            amount = jnp.sum(amount, axis=1, keepdims=True)
            some = amount > 0.0
            value = jnp.where(some, peak + jnp.log2(jnp.where(some, amount, 1.0)), FLOOR)
            values[...] = jnp.broadcast_to(value, (BATCH, LANES))

            def put(i, _):
                at = chosen[i].astype(jnp.float32)
                out[0:lines, :] = jnp.where(place == at, values[pl.ds(i, 1), :], out[0:lines, :])
                return 0

            lax.fori_loop(0, here, put, 0)
            return 0

        lax.fori_loop(0, (count + BATCH - 1) // BATCH, rescue, 0)


def finish_kernel(members, rows, me, gathered, loss_out, totals_out):
    weighted = jnp.zeros((rows, LANES), jnp.float32)
    counted = jnp.zeros((rows, LANES), jnp.float32)
    own = jnp.zeros((rows, LANES), jnp.float32)
    for owner in range(members):
        positive = gathered[owner, members * rows : (members + 1) * rows, :]
        weight = gathered[owner, (members + 1) * rows : (members + 2) * rows, :]
        shares = [
            gathered[k, (owner ^ k) * rows : ((owner ^ k) + 1) * rows, :] for k in range(members)
        ]
        peak = positive
        for share in shares:
            peak = jnp.maximum(peak, share)
        total = jnp.exp2(positive - peak)
        for share in shares:
            total = total + jnp.exp2(share - peak)
        loss = (peak - positive + jnp.log2(total)) * (1.0 / LOG2E)
        loss = jnp.where(weight > 0.0, loss, 0.0)
        weighted = weighted + weight * loss
        counted = counted + weight
        own = jnp.where(me[0] == owner, loss, own)
    loss_out[...] = own
    first = jnp.sum(weighted, axis=0, keepdims=True)
    second = jnp.sum(counted, axis=0, keepdims=True)
    line = lax.broadcasted_iota(jnp.int32, (8, LANES), 0)
    totals_out[...] = jnp.where(line == 0, first, jnp.where(line == 1, second, 0.0))


def mean_kernel(totals, received, out):
    totals = totals[...] + received[...]
    weighted = jnp.sum(totals[0:1], axis=1, keepdims=True)
    out[...] = weighted / jnp.sum(totals[1:2], axis=1, keepdims=True)


def call(kernel, shapes, *args, cost=None, scratch=(), smem=0, far=(), limit=16):
    specs = [SMEM] * smem + [VMEM] * (len(args) - smem)
    args = list(args)
    for place in far:
        specs[place] = HBM
        args[place] = pltpu.with_memory_space_constraint(args[place], pltpu.HBM)
    return pl.pallas_call(
        kernel,
        out_shape=shapes,
        in_specs=specs,
        out_specs=jax.tree.map(lambda _: VMEM, shapes),
        scratch_shapes=list(scratch),
        compiler_params=pltpu.CompilerParams(vmem_limit_bytes=limit * 2**20),
        cost_estimate=cost,
    )(*args)


def exchanged(value, axis, size, mask):
    return lax.ppermute(value, axis, [(i, i ^ mask) for i in range(size)])


def shards(
    dp,
    members,
    user_embed,
    positive_embed,
    positive_ids,
    token_weights,
    offsets,
    negative_embed,
    negative_ids,
):
    tokens, width = user_embed.shape
    number = negative_embed.shape[0]
    rows = tokens // LANES
    scale2 = 3.0 / math.sqrt(width) * LOG2E
    me = lax.axis_index("neg").reshape(1).astype(jnp.int32)
    id_rows = negative_ids.reshape(number // LANES, LANES)
    f32 = lambda *shape: jax.ShapeDtypeStruct(shape, jnp.float32)

    def cost(count):
        return pl.CostEstimate(
            flops=2 * count * tokens * number * width,
            bytes_accessed=number * width * 2,
            transcendentals=count * tokens * number,
        )

    like = lambda array: jax.ShapeDtypeStruct(array.shape, array.dtype)
    pack, targets, live, id_rows = call(
        pack_kernel,
        (
            jax.ShapeDtypeStruct((tokens + ID_ROWS, width), user_embed.dtype),
            like(positive_embed),
            f32(rows, LANES),
            like(id_rows),
        ),
        me,
        user_embed,
        positive_ids.reshape(rows, LANES),
        positive_embed,
        token_weights.reshape(rows, LANES),
        id_rows,
        offsets,
        smem=1,
        far=range(1, 7),
        scratch=[
            pltpu.VMEM((rows, LANES), jnp.int32),
            pltpu.VMEM((rows, LANES), jnp.int32),
            pltpu.SMEM(offsets.shape, jnp.int32),
            pltpu.SemaphoreType.DMA((6,)),
        ],
        limit=4,
    )
    packs = [pack] + [None] * (members - 1)
    for bit in reversed(range((members - 1).bit_length())):
        packs[2**bit] = exchanged(pack, "neg", members, 2**bit)
    shares, side, negatives = call(
        functools.partial(first_kernel, scale2),
        (
            f32(2 * rows, LANES),
            f32(2 * rows, LANES),
            like(negative_embed),
        ),
        *packs[:2],
        targets,
        live,
        id_rows,
        negative_embed,
        far=(5,),
        cost=cost(2),
        scratch=[pltpu.SemaphoreType.DMA((3,))],
    )
    early = [shares]
    for mask in range(2, members):
        if packs[mask] is None:
            low = mask & -mask
            source, early[0] = lax.optimization_barrier((packs[mask ^ low], early[0]))
            packs[mask] = exchanged(source, "neg", members, low)
    for mask in range(2, members - 1):
        early.append(
            call(
        functools.partial(sums_kernel, scale2),
        f32(rows, LANES),
        packs[mask],
        negatives,
        id_rows,
        cost=cost(1),
            )
        )
    lines = members * rows
    payload = call(
        functools.partial(last_kernel, scale2, members),
        f32(lines + 2 * rows, LANES),
        *packs,
        negatives,
        id_rows,
        *early,
        side,
        cost=cost(1),
        scratch=[
            pltpu.VMEM((lines, LANES), jnp.float32),
            pltpu.SMEM((BATCH,), jnp.int32),
            pltpu.VMEM((BATCH, width), jnp.float32),
            pltpu.VMEM((BATCH, LANES), jnp.float32),
            pltpu.VMEM((number // LANES, BATCH, LANES), jnp.float32),
            pltpu.VMEM((BATCH, LANES), jnp.float32),
            pltpu.VMEM((lines, LANES), jnp.float32),
        ],
    )
    gathered = lax.all_gather(payload, "neg", axis=0)
    loss, totals = call(
        functools.partial(finish_kernel, members, rows),
        (f32(rows, LANES), f32(8, LANES)),
        me,
        gathered,
        smem=1,
        limit=2,
    )
    mask = 1
    while mask < dp:
        received = exchanged(totals, "dp", dp, mask)
        mask *= 2
        if mask < dp:
            totals = totals + received
    mean = call(mean_kernel, f32(1, 1), totals, received, limit=1)
    return (loss.reshape(tokens), mean.reshape(()))


def solution(mesh):
    dp, members = mesh.shape["dp"], mesh.shape["neg"]
    in_specs = (
        P(("dp", "neg"), None),
        P(("dp", "neg"), None),
        P(("dp", "neg")),
        P(("dp", "neg")),
        P("dp", None),
        P("neg", None),
        P("neg"),
    )
    out_specs = (P(("dp", "neg")), P())
    return jax.shard_map(
        functools.partial(shards, dp, members),
        mesh=mesh,
        in_specs=in_specs,
        out_specs=out_specs,
        check_vma=False,
    )
```
